256 devices in a mesh: section: 4 (over y_lo, core), expert: 64 (over y_hi, x, z).
Axes of the slice: x: 4, y: 4 (y_hi: 2, y_lo: 2; y = y_hi * 2 + y_lo), z: 8, core: 2. Of those that a mesh axis runs over, the one named last changes fastest.
Arguments:
- activations: bfloat16 [4, 2048, 4096], P('section', 'expert'), may hold values from -6 to 6
- norm_gain: float32 [4, 4096], P('section'), may hold values from 0.25 to 1.75
- in_proj: bfloat16 [4, 4096, 40960], P('section', None, 'expert'), may hold values from -0.09375 to 0.09375
- out_proj: bfloat16 [4, 40960, 4096], P('section', 'expert'), may hold values from -0.078125 to 0.078125
- expert_ids: int32 [4, 2048, 1], P('section', 'expert'), may hold values from 0 to 7; in each aligned block of 32 rows (0 to 31, 32 to 63, ..., all dimensions but the last counted through in order) at most 8 rows name the same one
Outputs:
- passed: bfloat16 [4, 2048, 4096], P('section', 'expert')
The draws below stay inside these ranges and needn't reach their ends.
Inputs may be any that keep to these rules, and one draw needn't show every extreme that they name: `expert_ids`: within the 32 rows of one device (aligned blocks of 32 rows along the token dimension of each layer), no expert is named by more than 8 rows.
All inputs are finite; a program needn't handle non-finite values.
Results may differ from the reference program's by a relative error of at most 0.0047.
Values may be sent and summed in bfloat16 or wider, within the bound.
No kernel may reach another device: no remote copies, remote signals or barrier semaphores. Data moves between devices by JAX's collectives and lax.ppermute only.
A program may use at most 64 MiB of HBM per device.

```python
import math
import jax
import jax.numpy as jnp
import numpy as np
from jax import lax

D = 4096
FF_W = 5120
EXPERTS = 8
MB_TOK = 32
CAP = 8
TOKENS = 2048
N_SECTION = 4
N_EXPERT = 64


def steps_of(stream_key, dims, split, smallest, largest):
    gain, own = 1.0, jax.random.fold_in(stream_key, 6)
    for dim, parts in split:
        steps = jnp.exp(jax.random.uniform(jax.random.fold_in(own, dim), (parts,), jnp.float32, smallest / len(split), largest / len(split)))
        gain = gain * jnp.repeat(steps, dims[dim] // parts).reshape([-1 if axis == dim else 1 for axis in range(len(dims))])
    return gain


def shared_out(own_key, own, number, rows, number_of, top, bound, lean):
    order = jax.random.permutation(own_key, number_of)
    heavy_load, common = portions_of(number_of, rows * top, bound, lean, True), portions_of(number_of, rows * top, bound, lean, False)
    places = jnp.arange(number_of)

    def named(lengths, turn):
        used = int((lengths > 0).sum())
        fixed = max(1, used // 4)
        shifted = fixed + (places - fixed + turn * (used - fixed)) % max(1, number_of - fixed)
        return jnp.zeros((number_of,), jnp.int32).at[order[jnp.where(places < fixed, places, shifted)]].set(jnp.asarray(lengths, jnp.int32))

    lengths = jnp.where(number % 4 == 0, named(heavy_load, number // 4), named(common, number - number // 4 - 1))
    mixed = jax.random.permutation(jax.random.fold_in(own, 3), number_of)
    source_of, sink = mixed[0:number_of // 2 * 2:2], mixed[1:number_of // 2 * 2:2]
    margin = jnp.minimum(lengths[source_of] - 1, bound - lengths[sink]) // 2
    margin = jnp.where((source_of == order[0]) | (sink == order[0]) | (lengths[sink] == 0), 0, jnp.maximum(margin, 0))
    shifted = jax.random.randint(jax.random.fold_in(own, 4), (number_of // 2,), 0, 1 << 20) % (margin + 1)
    lengths = lengths.at[source_of].add(-shifted).at[sink].add(shifted)
    members = jnp.searchsorted(jnp.cumsum(lengths), jnp.arange(rows * top), side="right").astype(jnp.int32)
    listing = members.reshape(top, rows).T
    listing = listing[jax.random.permutation(jax.random.fold_in(own, 1), rows)]
    turn = jax.random.randint(jax.random.fold_in(own, 2), (rows, 1), 0, top)
    return jnp.take_along_axis(listing, (jnp.arange(top)[None, :] + turn) % top, axis=1)


def portions_of(count, total, most, slope, full):
    portions = [(1 << 20) // math.isqrt(grade ** slope) + 1 for grade in range(1, count + 1)]
    largest = most if full else min(most, max(-(-total // count), total * portions[0] // sum(portions)))
    least = 1 if total - largest >= count - 1 else 0
    given, spare = [largest] + [least] * (count - 1), total - largest - least * (count - 1)
    while spare > 0:
        candidates = [i for i in range(1, count) if given[i] < largest] or [i for i in range(1, count) if given[i] < most]
        mass, remaining = sum([portions[i] for i in candidates]), spare
        for i in candidates:
            extra = min(most - given[i], max(1, remaining * portions[i] // mass), spare)
            given[i] = given[i] + extra
            spare = spare - extra
    return np.array(given)


def centred(key, shape, width, most, shards=(), kind=jnp.bfloat16):
    factor_of = steps_of(key, shape, shards, -0.22, 0.18) if shards else 1.0
    drawn = jax.random.normal(key, shape, jnp.float32) * width * factor_of
    return jnp.minimum(jnp.maximum(drawn, -most), most).astype(kind)


def setup_inputs(seed: int = 0) -> dict:
    key_list = jax.random.split(jax.random.key(seed), 6)
    activations = centred(key_list[0], (N_SECTION, TOKENS, D), 1.0, 6.0, ((0, 4), (1, 64)))
    norm_gain = jnp.clip(1.0 + 0.15 * jax.random.normal(key_list[1], (N_SECTION, D), jnp.float32), 0.25, 1.75)
    in_proj = centred(key_list[2], (N_SECTION, D, EXPERTS * FF_W), D ** -0.5, 0.09375, ((0, 4), (2, 64)))
    out_proj = centred(key_list[3], (N_SECTION, EXPERTS * FF_W, D), FF_W ** -0.5, 0.078125, ((0, 4), (1, 64)))
    expert_ids_keys = jax.random.split(jax.random.fold_in(key_list[4], 1), N_SECTION * TOKENS // MB_TOK)
    expert_ids_turns = jax.random.permutation(jax.random.fold_in(key_list[4], 3), N_SECTION * TOKENS // MB_TOK)
    expert_ids = jax.vmap(lambda own, number: shared_out(jax.random.fold_in(key_list[4], 2), own, number, MB_TOK, EXPERTS, 1, CAP, 2))(expert_ids_keys, expert_ids_turns).reshape((N_SECTION, TOKENS, 1))
    return {"activations": activations, "norm_gain": norm_gain, "in_proj": in_proj, "out_proj": out_proj, "expert_ids": expert_ids}


epsilon = 1e-06

def reference(activations, norm_gain, in_proj, out_proj, expert_ids):
    groups = N_EXPERT // EXPERTS
    slice_width = FF_W // groups
    results = []
    for section_index in range(N_SECTION):
        floats = activations[section_index].astype(jnp.float32)
        scale = lax.rsqrt(lax.optimization_barrier(jnp.mean(floats * floats, axis=-1, keepdims=True)) + epsilon)
        normed = (floats * scale * norm_gain[section_index][None, :]).astype(jnp.bfloat16)
        routed = expert_ids[section_index, :, 0].astype(jnp.int32)
        onehot = (routed[:, None] == jnp.arange(EXPERTS, dtype=jnp.int32)[None, :]).astype(jnp.int32)
        blocked = onehot.reshape(N_EXPERT, MB_TOK, EXPERTS)
        before = (jnp.cumsum(blocked, axis=1) - blocked).reshape(TOKENS, EXPERTS)
        ranks = lax.optimization_barrier(jnp.sum(before * onehot, axis=1)).astype(jnp.int32)
        slots = (jnp.arange(TOKENS, dtype=jnp.int32) // MB_TOK * CAP + ranks).astype(jnp.int32)
        buffer = jnp.zeros((EXPERTS, N_EXPERT * CAP, D), jnp.bfloat16).at[routed, slots].set(normed)
        first_proj = in_proj[section_index].reshape(D, EXPERTS, FF_W).transpose(1, 0, 2)
        second_proj = out_proj[section_index].reshape(EXPERTS, FF_W, D)

        def expert(operands):
            inputs, first, second = operands
            preact = jnp.dot(inputs, first, preferred_element_type=jnp.float32)
            hidden = jax.nn.gelu(preact, approximate=True).astype(jnp.bfloat16)
            summed = jnp.zeros((inputs.shape[0], D), jnp.float32)
            for shard in range(groups):
                piece = jnp.dot(hidden[:, shard * slice_width:(shard + 1) * slice_width], second[shard * slice_width:(shard + 1) * slice_width], preferred_element_type=jnp.float32)
                summed = summed + piece
            return summed
        outputs = lax.map(expert, (buffer, first_proj, second_proj))
        mixed_rows = outputs[routed, slots]
        results.append((floats + mixed_rows).astype(jnp.bfloat16))
    return jnp.roll(jnp.stack(results), 1, axis=0)
```

```python
import jax
import jax.numpy as jnp
from jax import lax
from jax.sharding import PartitionSpec as P

EXPERTS = 8
LANES = 128

RAW_IN = 0
RAW_OUT = 0


epsilon = 1e-06


def from_behind(block, axis, distance):
    devices = range(lax.axis_size(axis))
    route = [((i - distance) % len(devices), i) for i in devices]
    return lax.ppermute(block, axis, route)


def around(block, groups, step):
    devices = range(lax.axis_size("expert"))
    route = [(i, i - i % groups + (i + step) % groups) for i in devices]
    return lax.ppermute(block, "expert", route)


def across(blocks, groups):
    members = [[e * groups + r for e in range(EXPERTS)] for r in range(groups)]
    return lax.all_to_all(
        blocks, "expert", split_axis=0, concat_axis=0, axis_index_groups=members, tiled=True
    )


def gather_ring(block, groups):
    half = groups // 2
    rows = block.shape[0] // 2
    blocks = [None] * groups
    blocks[0] = block
    ahead = behind = block
    for step in range(1, half):
        behind = around(behind, groups, 1)
        ahead = around(ahead, groups, -1)
        blocks[groups - step] = behind
        blocks[step] = ahead
    blocks[half] = jnp.concatenate(
        [around(behind[:rows], groups, 1), around(ahead[rows:], groups, -1)], axis=0
    )
    return blocks


def scatter_ring(parts, groups):
    half = groups // 2
    far = parts[half]()
    rows = far.shape[0] // 2
    zeros = jnp.zeros_like(far[:rows])
    right = around(far[:rows].astype(jnp.bfloat16), groups, 1).astype(jnp.float32)
    left = around(far[rows:].astype(jnp.bfloat16), groups, -1).astype(jnp.float32)
    right = jnp.concatenate([right, zeros], axis=0)
    left = jnp.concatenate([zeros, left], axis=0)
    for step in range(half - 1, 0, -1):
        right = around((right + parts[step]()).astype(jnp.bfloat16), groups, 1).astype(jnp.float32)
        left = around((left + parts[groups - step]()).astype(jnp.bfloat16), groups, -1).astype(
            jnp.float32
        )
    return right + left + parts[0]()


def matmul(a, b):
    return jnp.dot(a, b, preferred_element_type=jnp.float32)


def per_device(activations, norm_gain, in_proj, out_proj, expert_ids):
    floats = activations[0].astype(jnp.float32)
    tokens, width = floats.shape
    scale = lax.rsqrt(jnp.mean(floats * floats, axis=-1, keepdims=True) + epsilon)
    normed = (floats * scale * norm_gain[0][None, :]).astype(jnp.bfloat16)
    groups = lax.axis_size("expert") // EXPERTS
    capacity = 2 * tokens // EXPERTS
    slots = EXPERTS * capacity
    routed = expert_ids[0, :, 0]
    onehot = (routed[:, None] == jnp.arange(EXPERTS, dtype=jnp.int32)[None, :]).astype(jnp.int32)
    before = jnp.cumsum(onehot, axis=0) - onehot
    ranks = jnp.sum(before * onehot, axis=1)
    slot_index = (routed * capacity + ranks).astype(jnp.bfloat16)
    numbers = jnp.arange(slots, dtype=jnp.int32).astype(jnp.bfloat16)

    def placing_of(slot):
        return (slot[:, None] == numbers[None, :]).astype(jnp.bfloat16)

    def pack(placing, rows):
        return lax.dot_general(
            placing, rows, (((0,), (0,)), ((), ())), preferred_element_type=jnp.float32
        ).astype(jnp.bfloat16)

    placing = placing_of(slot_index)
    first_proj = in_proj[0]
    second_proj = out_proj[0]
    sorted_in, sorted_out = width - RAW_IN, width - RAW_OUT
    raw = RAW_IN or RAW_OUT

    if raw:
        tag = jnp.broadcast_to(slot_index[:, None], (tokens, LANES))
        ring = gather_ring(jnp.concatenate([normed[:, sorted_in:], tag], axis=1), groups)
        placings = [placing_of(block[:, RAW_IN]) for block in ring]
    received = across(pack(placing, normed[:, :sorted_in]), groups)
    flat = jnp.concatenate(gather_ring(received, groups), axis=0)
    preact = matmul(flat, first_proj[:sorted_in])
    if RAW_IN:
        packs = [pack(p, block[:, :RAW_IN]) for p, block in zip(placings, ring)]
        packs = jnp.stack([p.reshape(EXPERTS, capacity, RAW_IN) for p in packs], axis=1)
        rest = across(packs, groups).reshape(-1, RAW_IN)
        rest = matmul(rest, first_proj[sorted_in:]).reshape(EXPERTS, groups, capacity, -1)
        preact = preact + rest.transpose(1, 0, 2, 3).reshape(preact.shape)
    hidden = jax.nn.gelu(preact, approximate=True).astype(jnp.bfloat16)
    rows = [hidden[o * slots:(o + 1) * slots] for o in range(groups)]

    outputs = []
    if RAW_OUT:
        piece = matmul(hidden, second_proj[:, sorted_out:]).astype(jnp.bfloat16)
        piece = piece.reshape(groups, EXPERTS, capacity, RAW_OUT).transpose(1, 0, 2, 3)
        back = across(piece, groups)
        terms = [
            lambda o=o: matmul(placings[o], back[:, o].reshape(slots, RAW_OUT)) for o in range(groups)
        ]
    terms_sorted = [lambda o=o: matmul(rows[o], second_proj[:, :sorted_out]) for o in range(groups)]
    returned = across(scatter_ring(terms_sorted, groups).astype(jnp.bfloat16), groups)
    mixed = matmul(placing, returned)
    if RAW_OUT:
        mixed = jnp.concatenate([mixed, scatter_ring(terms, groups)], axis=1)
    updated = (floats + mixed).astype(jnp.bfloat16)
    return from_behind(updated[None], "section", 1)


def solution(mesh):
    return jax.shard_map(
        per_device,
        mesh=mesh,
        in_specs=(
            P("section", "expert", None),
            P("section", None),
            P("section", None, "expert"),
            P("section", "expert", None),
            P("section", "expert", None),
        ),
        out_specs=P("section", "expert", None),
        check_vma=False,
    )
```
